128 devices in a mesh: fsdp: 64 (over z, y, x), ep: 2 (over core).
Axes of the slice: x: 4, y: 4, z: 4, core: 2. Of those that a mesh axis runs over, the one named last changes fastest.
Arguments:
- x_tok: bfloat16 [262144, 512], P(('fsdp', 'ep'))
- dy_tok: bfloat16 [262144, 512], P(('fsdp', 'ep'))
- expert_idx: int32 [262144, 4], P(('fsdp', 'ep'))
- gate_val: float32 [262144, 4], P(('fsdp', 'ep'))
- w_one: bfloat16 [60, 512, 352], P('ep', 'fsdp')
- w_two: bfloat16 [60, 352, 512], P('ep', None, 'fsdp')
- w_three: bfloat16 [60, 512, 352], P('ep', 'fsdp')
- ws_one: bfloat16 [512, 1408], P('fsdp')
- ws_two: bfloat16 [1408, 512], P(None, 'fsdp')
- ws_three: bfloat16 [512, 1408], P('fsdp')
Outputs:
- output 1: bfloat16 [262144, 512], P(('fsdp', 'ep'))
- output 2: float32 [262144, 4], P(('fsdp', 'ep'))
- output 3: float32 [60, 512, 352], P('ep', 'fsdp')
- output 4: float32 [60, 352, 512], P('ep', None, 'fsdp')
- output 5: float32 [60, 512, 352], P('ep', 'fsdp')
- output 6: float32 [512, 1408], P('fsdp')
- output 7: float32 [1408, 512], P(None, 'fsdp')
- output 8: float32 [512, 1408], P('fsdp')
All inputs are finite; a program needn't handle non-finite values.
Results may differ from the reference program's by a relative error of at most 0.0058101.
Values are sent between devices in bfloat16 or wider.
A program may use at most 1 GiB of HBM per device.

```python
import jax
import jax.numpy as jnp
from jax import lax

MODEL_DIM = 512
EXPERT_FF = 352
SHARED_FF = 1408
EXPERTS = 60
TOP_K = 4
TOK_DEV = 2048
SRC_DEVICES = 128
CAPACITY = 176

TOKENS = TOK_DEV * SRC_DEVICES


def draw_routing(key):
    key_list = jax.random.split(key, 5)
    spread = EXPERTS // TOP_K
    jitter = max(spread // 4, 1)
    hot_span = max(EXPERTS // 8, 1)
    hot_start = jax.random.randint(key_list[0], (), 0, EXPERTS)
    is_hot = jax.random.randint(key_list[1], (TOKENS, 1), 0, 4) == 0
    base_hot = hot_start + jax.random.randint(key_list[2], (TOKENS, 1), 0, hot_span)
    base_any = jax.random.randint(key_list[3], (TOKENS, 1), 0, EXPERTS)
    base_id = jnp.where(is_hot, base_hot, base_any)
    offsets = jnp.arange(TOP_K, dtype=jnp.int32)[None, :] * spread + jax.random.randint(key_list[4], (TOKENS, TOP_K), 0, jitter)
    return ((base_id + offsets) % EXPERTS).astype(jnp.int32)


def setup_inputs(seed: int = 0) -> dict:
    key_list = jax.random.split(jax.random.key(seed), 10)
    dim_scale = MODEL_DIM ** -0.5
    ff_scale = EXPERT_FF ** -0.5
    shared_scale = SHARED_FF ** -0.5
    x_tok = jax.random.normal(key_list[0], (TOKENS, MODEL_DIM), jnp.float32).astype(jnp.bfloat16)
    dy_tok = jax.random.normal(key_list[1], (TOKENS, MODEL_DIM), jnp.float32).astype(jnp.bfloat16)
    expert_idx = draw_routing(key_list[2])
    gate_val = jax.random.uniform(key_list[3], (TOKENS, TOP_K), jnp.float32, 0.3, 1.0)
    w_one = (jax.random.normal(key_list[4], (EXPERTS, MODEL_DIM, EXPERT_FF), jnp.float32) * dim_scale).astype(jnp.bfloat16)
    w_two = (jax.random.normal(key_list[5], (EXPERTS, EXPERT_FF, MODEL_DIM), jnp.float32) * ff_scale).astype(jnp.bfloat16)
    w_three = (jax.random.normal(key_list[6], (EXPERTS, MODEL_DIM, EXPERT_FF), jnp.float32) * dim_scale).astype(jnp.bfloat16)
    ws_one = (jax.random.normal(key_list[7], (MODEL_DIM, SHARED_FF), jnp.float32) * dim_scale).astype(jnp.bfloat16)
    ws_two = (jax.random.normal(key_list[8], (SHARED_FF, MODEL_DIM), jnp.float32) * shared_scale).astype(jnp.bfloat16)
    ws_three = (jax.random.normal(key_list[9], (MODEL_DIM, SHARED_FF), jnp.float32) * dim_scale).astype(jnp.bfloat16)
    return {"x_tok": x_tok, "dy_tok": dy_tok, "expert_idx": expert_idx, "gate_val": gate_val, "w_one": w_one, "w_two": w_two, "w_three": w_three, "ws_one": ws_one, "ws_two": ws_two, "ws_three": ws_three}


def slots_for_source(ids_src):
    flat_ids = ids_src.reshape(-1)
    onehot = (flat_ids[:, None] == jnp.arange(EXPERTS, dtype=jnp.int32)[None, :]).astype(jnp.int32)
    slot_pos = jnp.sum(jnp.cumsum(onehot, axis=0) * onehot, axis=1) - 1
    return jnp.where(slot_pos < CAPACITY, flat_ids * CAPACITY + slot_pos, EXPERTS * CAPACITY)


def fill_for_source(slot_idx):
    n_assign = TOK_DEV * TOP_K
    filled = jnp.full((EXPERTS * CAPACITY + 1,), n_assign, jnp.int32)
    filled = filled.at[slot_idx].set(jnp.arange(n_assign, dtype=jnp.int32))
    return filled[: EXPERTS * CAPACITY]


def swiglu_grads(x_rows, g_rows, w_a, w_b, w_c):
    h_one = jnp.dot(x_rows, w_a, preferred_element_type=jnp.float32)
    h_three = jnp.dot(x_rows, w_c, preferred_element_type=jnp.float32)
    sig_one = jax.nn.sigmoid(h_one)
    silu_one = h_one * sig_one
    act_rows = (silu_one * h_three).astype(jnp.bfloat16)
    d_act = jnp.dot(g_rows, w_b.T, preferred_element_type=jnp.float32)
    dh_one = (d_act * h_three * sig_one * (1.0 + h_one * (1.0 - sig_one))).astype(jnp.bfloat16)
    dh_three = (d_act * silu_one).astype(jnp.bfloat16)
    dx_rows = (jnp.dot(dh_one, w_a.T, preferred_element_type=jnp.float32) + jnp.dot(dh_three, w_c.T, preferred_element_type=jnp.float32)).astype(jnp.bfloat16)
    dw_a = jnp.dot(x_rows.T, dh_one, preferred_element_type=jnp.float32)
    dw_b = jnp.dot(act_rows.T, g_rows, preferred_element_type=jnp.float32)
    dw_c = jnp.dot(x_rows.T, dh_three, preferred_element_type=jnp.float32)
    return dx_rows, act_rows, dw_a, dw_b, dw_c


def reference(x_tok, dy_tok, expert_idx, gate_val, w_one, w_two, w_three, ws_one, ws_two, ws_three):
    n_assign = TOK_DEV * TOP_K
    slot_idx = jax.vmap(slots_for_source)(expert_idx.reshape(SRC_DEVICES, TOK_DEV, TOP_K))
    filled = jax.vmap(fill_for_source)(slot_idx)
    src_base = jnp.arange(SRC_DEVICES, dtype=jnp.int32)[:, None] * n_assign
    global_ids = jnp.where(filled < n_assign, filled + src_base, TOKENS * TOP_K)
    expert_rows = global_ids.reshape(SRC_DEVICES, EXPERTS, CAPACITY).transpose(1, 0, 2).reshape(EXPERTS, SRC_DEVICES * CAPACITY)
    zero_row = jnp.zeros((1, MODEL_DIM), jnp.bfloat16)
    x_pad = jnp.concatenate([x_tok, zero_row])
    dy_pad = jnp.concatenate([dy_tok, zero_row])
    gate_pad = jnp.concatenate([gate_val.reshape(-1), jnp.zeros((1,), jnp.float32)])

    def expert_step(acc_state, step_in):
        dx_acc, dgate_acc = acc_state
        assign_ids, w_a, w_b, w_c = step_in
        tok_ids = assign_ids // TOP_K
        x_rows = x_pad[tok_ids]
        dy_rows = dy_pad[tok_ids]
        dy_wide = dy_rows.astype(jnp.float32)
        g_rows = (gate_pad[assign_ids][:, None] * dy_wide).astype(jnp.bfloat16)
        dx_rows, act_rows, dw_a, dw_b, dw_c = swiglu_grads(x_rows, g_rows, w_a, w_b, w_c)
        y_rows = jnp.dot(act_rows, w_b, preferred_element_type=jnp.float32)
        dgate_rows = jnp.sum(dy_wide * y_rows, axis=1)
        dx_acc = dx_acc.at[tok_ids].add(dx_rows.astype(jnp.float32))
        dgate_acc = dgate_acc.at[assign_ids].add(dgate_rows)
        return (dx_acc, dgate_acc), (dw_a, dw_b, dw_c)

    init_state = (jnp.zeros((TOKENS + 1, MODEL_DIM), jnp.float32), jnp.zeros((TOKENS * TOP_K + 1,), jnp.float32))
    final_state, expert_grads = lax.scan(expert_step, init_state, (expert_rows, w_one, w_two, w_three))

    def shared_step(acc_state, step_in):
        x_rows, dy_rows = step_in
        dx_rows, act_rows, dw_a, dw_b, dw_c = swiglu_grads(x_rows, dy_rows, ws_one, ws_two, ws_three)
        return (acc_state[0] + dw_a, acc_state[1] + dw_b, acc_state[2] + dw_c), dx_rows

    shared_init = (jnp.zeros((MODEL_DIM, SHARED_FF), jnp.float32), jnp.zeros((SHARED_FF, MODEL_DIM), jnp.float32), jnp.zeros((MODEL_DIM, SHARED_FF), jnp.float32))
    x_blocks = x_tok.reshape(SRC_DEVICES, TOK_DEV, MODEL_DIM)
    dy_blocks = dy_tok.reshape(SRC_DEVICES, TOK_DEV, MODEL_DIM)
    shared_grads, dx_shared = lax.scan(shared_step, shared_init, (x_blocks, dy_blocks))
    dx_acc, dgate_acc = final_state
    dx_out = (dx_acc[:TOKENS] + dx_shared.reshape(TOKENS, MODEL_DIM).astype(jnp.float32)).astype(jnp.bfloat16)
    dgate = dgate_acc[: TOKENS * TOP_K].reshape(TOKENS, TOP_K)
    return (dx_out, dgate, expert_grads[0], expert_grads[1], expert_grads[2], shared_grads[0], shared_grads[1], shared_grads[2])
```

```python
import jax
import jax.numpy as jnp
from jax import lax
from jax.sharding import Mesh
from jax.sharding import PartitionSpec as P

CAP_NUM = 5
CAP_DEN = 4
RING = 4


def capacity_for(tok_dev, top_k, n_exp):
    needed = -(-(tok_dev * top_k * CAP_NUM) // (CAP_DEN * n_exp))
    return max(8, -(-needed // 8) * 8)


def route(ids, n_exp, capacity):
    flat = ids.reshape(-1)
    n_assign = flat.shape[0]
    onehot = (flat[:, None] == jnp.arange(n_exp, dtype=jnp.int32)[None, :]).astype(jnp.int32)
    pos = jnp.sum(jnp.cumsum(onehot, axis=0) * onehot, axis=1) - 1
    kept = pos < capacity
    slot = jnp.where(kept, flat * capacity + pos, n_exp * capacity)
    filled = jnp.full((n_exp * capacity + 1,), n_assign, jnp.int32)
    filled = filled.at[slot].set(jnp.arange(n_assign, dtype=jnp.int32))
    return pos, kept, filled[: n_exp * capacity]


def swiglu_backward(x, dy, g, wa, wc, wbt, b):
    f32 = jnp.float32
    up = b + "td," + b + "df->" + b + "tf"
    back = b + "tf," + b + "df->" + b + "td"
    outer = b + "td," + b + "tf->" + b + "df"
    h1 = jnp.einsum(up, x, wa, preferred_element_type=f32)
    h3 = jnp.einsum(up, x, wc, preferred_element_type=f32)
    sig = jax.nn.sigmoid(h1)
    silu = h1 * sig
    a = (silu * h3).astype(jnp.bfloat16)
    da = jnp.einsum(up, g, wbt, preferred_element_type=f32)
    dh1 = (da * h3 * sig * (1.0 + h1 * (1.0 - sig))).astype(jnp.bfloat16)
    dh3 = (da * silu).astype(jnp.bfloat16)
    dx = (jnp.einsum(back, dh1, wa, preferred_element_type=f32) + jnp.einsum(back, dh3, wc, preferred_element_type=f32)).astype(jnp.bfloat16)
    dwa = jnp.einsum(outer, x, dh1, preferred_element_type=f32)
    dwc = jnp.einsum(outer, x, dh3, preferred_element_type=f32)
    dwbt = jnp.einsum(outer, g, a, preferred_element_type=f32)
    if dy is None:
        return dx, None, dwa, dwc, dwbt
    y = jnp.einsum(back, a, wbt, preferred_element_type=f32)
    dgate = jnp.sum(dy.astype(f32) * y, axis=-1)
    return dx, dgate, dwa, dwc, dwbt


def solution(mesh):
    n_fsdp, n_core = mesh.devices.shape
    plane = n_fsdp // RING
    mesh4 = Mesh(mesh.devices.reshape(RING, plane, n_core), ("z", "p", "core"))
    tok = P(("z", "p", "core"), None)
    in_specs = (tok, tok, tok, tok, P("core", ("z", "p"), None), P("core", None, ("z", "p")), P("core", ("z", "p"), None), P(("z", "p"), None), P(None, ("z", "p")), P(("z", "p"), None))
    out_specs = (tok, tok, P("core", ("z", "p"), None), P("core", None, ("z", "p")), P("core", ("z", "p"), None), P(("z", "p"), None), P(None, ("z", "p")), P(("z", "p"), None))

    def device_step(x, dy, ids, gate, w1, w2, w3, ws1, ws2, ws3):
        t, k = ids.shape
        d = x.shape[1]
        nl, dl, ff = w1.shape
        n_exp = nl * n_core
        cap = capacity_for(t, k, n_exp)
        eo = -(-nl // RING)
        nb = RING * n_core
        zi = lax.axis_index("z")
        ci = lax.axis_index("core")
        fsh = ws1.shape[1]

        wss = jnp.stack([ws1, ws3, ws2.T])
        wsg = lax.all_gather(wss, ("z", "p"), axis=1, tiled=True)
        wst = jnp.stack([w1, w3, w2.transpose(0, 2, 1)])
        wst = jnp.pad(wst, ((0, 0), (0, RING * eo - nl), (0, 0), (0, 0))).reshape(3, RING, eo, dl, ff)
        wz = lax.all_to_all(wst.transpose(1, 0, 2, 3, 4), "z", 0, 0, tiled=True)
        wz = wz.transpose(1, 2, 0, 3, 4)
        wg = lax.all_gather(wz, "p", axis=3, tiled=True).reshape(3, eo, d, ff)

        fwd = [(i, (i + 1) % RING) for i in range(RING)]
        bwd = [(i, (i - 1) % RING) for i in range(RING)]
        half = t // 2
        xs, dys = [], []
        for src, acc in ((x, xs), (dy, dys)):
            m1 = lax.ppermute(src, "z", bwd)
            p1 = lax.ppermute(src, "z", fwd)
            p2 = lax.ppermute(p1[:half], "z", fwd)
            m2 = lax.ppermute(m1[half:], "z", bwd)
            blocks = [src, m1, jnp.concatenate([p2, m2]), p1]
            for blk in blocks:
                acc.append(blk)
                acc.append(lax.ppermute(blk, "core", [(i, (i + 1) % n_core) for i in range(n_core)]))

        pos, kept, filled = route(ids, n_exp, cap)
        tokf = jnp.where(filled < t * k, filled // k, t).astype(jnp.float32)
        gatef = jnp.concatenate([gate.reshape(-1), jnp.zeros((1,), jnp.float32)])[filled]
        meta = jnp.stack([tokf, gatef]).reshape(2, n_core, nl, cap)
        meta = jnp.pad(meta, ((0, 0), (0, 0), (0, RING * eo - nl), (0, 0)), constant_values=float(0))
        meta = meta.reshape(2, n_core, RING, eo, cap).transpose(2, 1, 0, 3, 4).reshape(nb, 2, eo, cap)
        meta = lax.all_to_all(meta, ("z", "core"), 0, 0, tiled=True)
        rel = jnp.arange(nb, dtype=jnp.int32)
        order = ((zi + rel // n_core) % RING) * n_core + (ci + rel % n_core) % n_core
        meta = meta[order]
        tok_idx = meta[:, 0].astype(jnp.int32)
        gates = meta[:, 1].transpose(1, 0, 2).reshape(eo, nb * cap)

        xg = jnp.stack([xs[b].at[tok_idx[b]].get(mode="fill", fill_value=0) for b in range(nb)], axis=1).reshape(eo, nb * cap, d)
        dyg = jnp.stack([dys[b].at[tok_idx[b]].get(mode="fill", fill_value=0) for b in range(nb)], axis=1).reshape(eo, nb * cap, d)
        gg = (gates[..., None] * dyg.astype(jnp.float32)).astype(jnp.bfloat16)
        dxr, dgr, dwa, dwc, dwbt = swiglu_backward(xg, dyg, gg, wg[0], wg[1], wg[2], "e")

        dxr = dxr.reshape(eo, nb, cap, d)
        back = []
        for b in range(nb):
            kz, kc = b // n_core, b % n_core
            perm = [(z * n_core + c, ((z + kz) % RING) * n_core + (c + kc) % n_core) for z in range(RING) for c in range(n_core)]
            blk = dxr[:, b]
            back.append(blk if b == 0 else lax.ppermute(blk, ("z", "core"), perm))
        dx_back = jnp.concatenate([jnp.stack(back).reshape(nb * eo * cap, d), jnp.zeros((1, d), jnp.bfloat16)])
        dgr = dgr.reshape(eo, nb, cap).transpose(1, 0, 2)
        inv = ((rel // n_core - zi) % RING) * n_core + (rel % n_core + ci) % n_core
        dg_back = lax.all_to_all(dgr[inv], ("z", "core"), 0, 0, tiled=True).reshape(-1)

        flat = ids.reshape(-1)
        co, lo = flat // nl, flat % nl
        zo, io = lo // eo, lo % eo
        mrel = ((zi - zo) % RING) * n_core + (ci + co) % n_core
        slot = jnp.where(kept, (mrel * eo + io) * cap + pos, nb * eo * cap)
        slot_abs = jnp.where(kept, ((zo * n_core + co) * eo + io) * cap + pos, nb * eo * cap)
        dx_assign = dx_back[slot].reshape(t, k, d)
        dgate = jnp.concatenate([dg_back, jnp.zeros((1,), jnp.float32)])[slot_abs].reshape(t, k)

        dxs, _, dsa, dsc, dsbt = swiglu_backward(x, None, dy, wsg[0], wsg[1], wsg[2], "")
        dx = (jnp.sum(dx_assign.astype(jnp.float32), axis=1) + dxs.astype(jnp.float32)).astype(jnp.bfloat16)

        span = -(-fsh // (128 * n_core)) * 128
        off = fsh - span
        ds = jnp.stack([dsa, dsc, dsbt])
        mine = lax.dynamic_slice_in_dim(ds, ci * off, span, axis=2)
        other = lax.dynamic_slice_in_dim(ds, (1 - ci) * off, span, axis=2)
        mine = mine + lax.ppermute(other, "core", [(0, 1), (1, 0)])
        mine = lax.psum_scatter(mine, ("z", "p"), scatter_dimension=1, tiled=True)
        both = lax.all_gather(mine, "core")
        dsg = jnp.concatenate([both[0][..., :off], both[1]], axis=-1)

        def reduce(dw):
            return lax.psum_scatter(dw.reshape(eo, RING, d // RING, ff), "p", scatter_dimension=2, tiled=True)

        dws = jnp.stack([reduce(dwa), reduce(dwc), reduce(dwbt)])
        dws = lax.all_to_all(dws.transpose(2, 0, 1, 3, 4), "z", 0, 0, tiled=True)
        dws = dws.transpose(1, 0, 2, 3, 4).reshape(3, RING * eo, dl, ff)[:, :nl]
        return dx, dgate, dws[0], dws[2].transpose(0, 2, 1), dws[1], dsg[0], dsg[2].T, dsg[1]

    return jax.shard_map(device_step, mesh=mesh4, in_specs=in_specs, out_specs=out_specs, check_vma=False)
```
